32 devices in a mesh: rows: 8 (over y, x, core), feat: 4 (over z).
Axes of the slice: x: 2, y: 2, z: 4, core: 2. Of those that a mesh axis runs over, the one named last changes fastest.
Arguments:
- bins: int32 [16384, 1024], P('rows', 'feat'), may hold values from 0 to 255
- node_ids: int32 [2, 16384], P(None, 'rows'), may hold values from 0 to 15
- boot_counts: int32 [2, 16384], P(None, 'rows'), may hold values from 0 to 3
- gradient: bfloat16 [16384], P('rows'), may hold values from -6 to 6
Outputs:
- gains: float32 [4, 256, 2, 16, 256], P('feat', 'rows')
- best_gain: float32 [2, 16], replicated
The draws below stay inside these ranges and needn't reach their ends.
All inputs are finite; a program needn't handle non-finite values.
Results may differ from the reference program's by a relative error of at most 0.003.
Values may be sent and summed in bfloat16 or wider, within the bound.
A program may use at most 64 MiB of HBM per device.

```python
import math
import jax
import jax.numpy as jnp
import numpy as np

F = 1024
BINS = 256
TREES = 2
NODES = 16
ROWS = 16384
N_FEAT = 4


def with_ends(result, stream_key, low, top_value):
    longest = result.shape.index(max(result.shape))
    spots = []
    for shift in (0, 1):
        where = [jax.random.randint(jax.random.fold_in(stream_key, axis), (), 0, length) for axis, length in enumerate(result.shape)]
        where[longest] = (where[longest] + shift) % result.shape[longest]
        spots.append(tuple(where))
    return result.at[spots[0]].set(low).at[spots[1]].set(top_value)


def block_scale(rng, shape, split, least, high):
    level, own = 1.0, jax.random.fold_in(rng, 6)
    for axis_at, parts in split:
        heights = jnp.exp(jax.random.uniform(jax.random.fold_in(own, axis_at), (parts,), jnp.float32, least / len(split), high / len(split)))
        level = level * jnp.repeat(heights, shape[axis_at] // parts).reshape([-1 if axis == axis_at else 1 for axis in range(len(shape))])
    return level


def rank_table(count, lean):
    portions = [(1 << 20) // math.isqrt(standing ** lean) + 1 for standing in range(1, count + 1)]
    width = 1 + sum(portions) // (1 << 30)
    return np.cumsum(np.array([max(1, weight // width) for weight in portions]))


def skewed_ids(rng, shape, count, slope):
    table = rank_table(count, slope)
    lot = jax.random.randint(jax.random.fold_in(rng, 1), shape, 0, int(table[count - 1]))
    grade = jnp.searchsorted(jnp.asarray(table, jnp.int32), lot, side="right")
    return jax.random.permutation(jax.random.fold_in(rng, 2), count)[grade].astype(jnp.int32)


def bell_draw(stream_key, dims, deviation, bound, shards=(), kind=jnp.bfloat16):
    result = deviation * jax.random.normal(stream_key, dims, jnp.float32)
    if shards:
        result = result * block_scale(stream_key, dims, shards, -0.22, 0.18)
    return jnp.clip(result, -bound, bound).astype(kind)


def setup_inputs(seed: int = 0) -> dict:
    key_list = jax.random.split(jax.random.key(seed), 5)
    return {
        "bins": with_ends(jax.random.randint(key_list[0], (ROWS, F), 0, BINS), jax.random.fold_in(key_list[0], 1), 0, BINS - 1).astype(jnp.int32),
        "node_ids": with_ends(skewed_ids(key_list[1], (TREES, ROWS), NODES, 2), jax.random.fold_in(key_list[1], 3), 0, NODES - 1).astype(jnp.int32),
        "boot_counts": with_ends(jax.random.randint(key_list[2], (TREES, ROWS), 0, 4), jax.random.fold_in(key_list[2], 1), 0, 3).astype(jnp.int32),
        "gradient": bell_draw(key_list[3], (ROWS,), 1.0, 6.0, ((0, 8),)),
    }


ridge = 1.0


def split_gains(hist):
    left_grad = jnp.cumsum(hist[:, :, 0], axis=-1)
    left_count = jnp.cumsum(hist[:, :, 1], axis=-1)
    total_grad = left_grad[..., -1:]
    total_count = left_count[..., -1:]
    right_grad = total_grad - left_grad
    right_count = total_count - left_count
    return (left_grad * left_grad / (left_count + ridge)
            + right_grad * right_grad / (right_count + ridge)
            - total_grad * total_grad / (total_count + ridge))


def reference(bins, node_ids, boot_counts, gradient):
    weighted = (boot_counts.astype(jnp.float32) * gradient.astype(jnp.float32)[None, :]).astype(jnp.bfloat16)
    block = 128
    per_tree = []
    for tree in range(TREES):
        grad_vals = weighted[tree].astype(jnp.float32)
        count_vals = boot_counts[tree].astype(jnp.float32)
        blocks = []
        for block_start in range(0, F, block):
            picked = bins[:, block_start:block_start + block]
            segment_ids = (jnp.arange(block, dtype=jnp.int32)[None, :] * NODES + node_ids[tree][:, None]) * BINS + picked
            segment_ids = segment_ids.reshape(-1)
            total = block * NODES * BINS
            grad_hist = jax.ops.segment_sum(jnp.broadcast_to(grad_vals[:, None], picked.shape).reshape(-1), segment_ids, num_segments=total)
            count_hist = jax.ops.segment_sum(jnp.broadcast_to(count_vals[:, None], picked.shape).reshape(-1), segment_ids, num_segments=total)
            blocks.append(jnp.stack([grad_hist.reshape(block, NODES, BINS), count_hist.reshape(block, NODES, BINS)], axis=1))
        per_tree.append(jnp.concatenate(blocks, axis=0))
    hist = jnp.stack(per_tree, axis=1)
    gain = split_gains(hist)
    best_gain = jnp.max(gain, axis=(0, 3))
    gains = gain.reshape(N_FEAT, F // N_FEAT, TREES, NODES, BINS)
    return gains, best_gain
```

```python
import functools
import math

import jax
import jax.numpy as jnp
from jax import lax
from jax.experimental import pallas as pl
from jax.experimental.pallas import tpu as pltpu
from jax.sharding import PartitionSpec as P

BINS = 256
NODES = 16
RIDGE = 1.0
F8 = jnp.float8_e4m3fn
F32 = jnp.float32
BF16 = jnp.bfloat16
MESH = pl.DeviceIdType.MESH
NT = (((1,), (1,)), ((), ()))


def partner(me, step, count):
    if count & (count - 1):
        return lax.rem(me + step, count)
    out = me
    bit = 1
    while bit < count:
        if step & bit:
            out = out + bit * (1 - 2 * lax.rem(me // bit, 2))
        bit *= 2
    return out


def kernel(
    n, nf, trees, bins_ref, lab_ref, gains_ref, best_ref,
    got, labels, binsf, cols, acc, row_out, row_in,
    send_b, recv_b, send_l, recv_l, send_m, recv_m,
):
    _, owned, rows = bins_ref.shape
    wide = trees * NODES
    total = n * nf
    me, mf = lax.axis_index("rows"), lax.axis_index("feat")

    barrier = pltpu.get_barrier_semaphore()

    def greet(j, _):
        to = {"rows": lax.rem(me + j // nf, n), "feat": lax.rem(mf + j % nf, nf)}
        pl.semaphore_signal(barrier, inc=1, device_id=to, device_id_type=MESH)
        return 0

    lax.fori_loop(1, total, greet, 0)
    pl.semaphore_wait(barrier, total - 1)

    def label_copy(k, to):
        return pltpu.make_async_remote_copy(
            src_ref=lab_ref, dst_ref=labels.at[k], send_sem=send_l.at[k],
            recv_sem=recv_l.at[k], device_id={"rows": to}, device_id_type=MESH)

    def bins_copy(k, to):
        return pltpu.make_async_remote_copy(
            src_ref=bins_ref.at[to], dst_ref=got.at[k], send_sem=send_b.at[k],
            recv_sem=recv_b.at[k], device_id={"rows": to}, device_id_type=MESH)

    for k in range(1, n):
        to = partner(me, k, n)
        label_copy(k, to).start()
        bins_copy(k, to).start()

    got[0] = bins_ref[me]
    labels[0] = lab_ref[...]
    acc[...] = jnp.zeros_like(acc)

    chunk = math.gcd(512, rows)
    unroll = math.gcd(8, owned)
    edges = lax.broadcasted_iota(jnp.int32, (BINS, chunk), 0).astype(BF16)
    node_of = lax.broadcasted_iota(jnp.int32, (NODES, chunk), 0).astype(F32)
    one, zero = BF16(1), BF16(0)

    def block(k, _):
        @pl.when(k > 0)
        def _():
            to = lax.rem(me + 1, n)
            label_copy(k, to).wait_recv()
            bins_copy(k, to).wait_recv()

        binsf[...] = got[k].astype(F32)
        lab = labels[k].astype(F32)
        counts = lab[trees:2 * trees]
        weighted = (counts * lab[2 * trees:2 * trees + 1]).astype(BF16).astype(F32)
        for c in range(0, rows, chunk):
            span = slice(c, c + chunk)
            hot = [lab[t:t + 1, span] == node_of for t in range(trees)]

            def spread(values):
                return jnp.concatenate(
                    [jnp.where(hot[t], values[t:t + 1, span], 0.0) for t in range(trees)], axis=0)

            cols[0:wide, span] = spread(weighted).astype(BF16)
            cols[wide:2 * wide, span] = spread(counts).astype(BF16)

        def features(g, _):
            for u in range(unroll):
                f = g * unroll + u
                hist = None
                for c in range(0, rows, chunk):
                    row = binsf[pl.ds(f, 1), c:c + chunk].astype(BF16)
                    mask = jnp.where(row <= edges, one, zero).astype(F8)
                    part = lax.dot_general(
                        cols[:, c:c + chunk], mask, NT, preferred_element_type=F32)
                    hist = part if hist is None else hist + part
                acc[f] += hist
            return 0

        lax.fori_loop(0, owned // unroll, features, 0)
        return 0

    lax.fori_loop(0, n, block, 0)

    def finish(f, top):
        left_grad = acc[f, 0:wide]
        left_count = acc[f, wide:2 * wide]
        total_grad = left_grad[:, BINS - 1:BINS]
        total_count = left_count[:, BINS - 1:BINS]
        right_grad = total_grad - left_grad
        right_count = total_count - left_count
        gain = (
            left_grad * left_grad / (left_count + RIDGE)
            + right_grad * right_grad / (right_count + RIDGE)
            - total_grad * total_grad / (total_count + RIDGE)
        )
        gains_ref[f] = gain
        return jnp.maximum(top, gain)

    top = lax.fori_loop(0, owned, finish, jnp.full((wide, BINS), -jnp.inf, F32))
    top = jnp.max(top, axis=1, keepdims=True)
    diagonal = (
        lax.broadcasted_iota(jnp.int32, (wide, 128), 0)
        == lax.broadcasted_iota(jnp.int32, (wide, 128), 1)
    )
    row = jnp.max(jnp.where(diagonal, top, -jnp.inf), axis=0, keepdims=True)
    row_out[...] = row
    row_in[0] = row

    def row_copy(j):
        to = {"rows": lax.rem(me + j // nf, n), "feat": lax.rem(mf + j % nf, nf)}
        return pltpu.make_async_remote_copy(
            src_ref=row_out, dst_ref=row_in.at[j], send_sem=send_m.at[j],
            recv_sem=recv_m.at[j], device_id=to, device_id_type=MESH)

    def send_row(j, _):
        row_copy(j).start()
        return 0

    lax.fori_loop(1, total, send_row, 0)

    for k in range(1, n):
        to = partner(me, k, n)
        label_copy(k, to).wait_send()
        bins_copy(k, to).wait_send()

    def take_row(j, _):
        row_copy(j).wait_send()
        row_copy(j).wait_recv()
        return 0

    lax.fori_loop(1, total, take_row, 0)
    best_ref[...] = jnp.max(row_in[...], axis=0)


def per_device(n, nf, bins, node_ids, boot_counts, gradient):
    rows, feat_local = bins.shape
    trees = node_ids.shape[0]
    owned = feat_local // n
    wide = trees * NODES
    by_owner = bins.astype(BF16).T.reshape(n, owned, rows)
    labels = jnp.concatenate(
        [node_ids.astype(BF16), boot_counts.astype(BF16), gradient[None]], axis=0)
    tall = -(-labels.shape[0] // 8) * 8
    labels = jnp.pad(labels, ((0, tall - labels.shape[0]), (0, 0)))
    total = n * nf
    vmem = pl.BlockSpec(memory_space=pltpu.VMEM)
    gains, best = pl.pallas_call(
        functools.partial(kernel, n, nf, trees),
        out_shape=(
            jax.ShapeDtypeStruct((owned, wide, BINS), F32),
            jax.ShapeDtypeStruct((1, 128), F32),
        ),
        in_specs=[vmem, vmem],
        out_specs=(vmem, vmem),
        scratch_shapes=[
            pltpu.VMEM((n, owned, rows), BF16),
            pltpu.VMEM((n, tall, rows), BF16),
            pltpu.VMEM((owned, rows), F32),
            pltpu.VMEM((2 * wide, rows), BF16),
            pltpu.VMEM((owned, 2 * wide, BINS), F32),
            pltpu.VMEM((1, 128), F32),
            pltpu.VMEM((total, 1, 128), F32),
            pltpu.SemaphoreType.DMA((n,)),
            pltpu.SemaphoreType.DMA((n,)),
            pltpu.SemaphoreType.DMA((n,)),
            pltpu.SemaphoreType.DMA((n,)),
            pltpu.SemaphoreType.DMA((total,)),
            pltpu.SemaphoreType.DMA((total,)),
        ],
        compiler_params=pltpu.CompilerParams(
            collective_id=0, has_side_effects=True, vmem_limit_bytes=48 * 2**20),
    )(by_owner, labels)
    gains = gains.reshape(1, owned, trees, NODES, BINS)
    return gains, best[0, :wide].reshape(trees, NODES)


def solution(mesh):
    n, nf = mesh.shape["rows"], mesh.shape["feat"]
    in_specs = (P("rows", "feat"), P(None, "rows"), P(None, "rows"), P("rows"))
    out_specs = (P("feat", "rows", None, None, None), P())
    return jax.shard_map(
        functools.partial(per_device, n, nf),
        mesh=mesh, in_specs=in_specs, out_specs=out_specs, check_vma=False)
```
